256 devices in a mesh: dp: 8 (over z), expert: 32 (over y, x, core).
Axes of the slice: x: 4, y: 4, z: 8, core: 2. Of those that a mesh axis runs over, the one named last changes fastest.
Arguments:
- tokens: bfloat16 [1024, 7168], P(('dp', 'expert')), may hold values from -6 to 6
- routes: int32 [1024, 8], P(('dp', 'expert')), may hold values from 0 to 31, all different within a row; in each aligned block of 4 rows (0 to 3, 4 to 7, ...) at most 2 rows name the same one
- gate_scores: float32 [1024, 8], P(('dp', 'expert')), may hold values from 0.1 to 1
- w_gate: bfloat16 [32, 7168, 2048], P('expert', None, 'dp'), may hold values from -0.0625 to 0.0625
- w_up: bfloat16 [32, 7168, 2048], P('expert', None, 'dp'), may hold values from -0.0625 to 0.0625
- w_down: bfloat16 [32, 2048, 7168], P('expert', 'dp'), may hold values from -0.125 to 0.125
Outputs:
- mixed_out: bfloat16 [1024, 7168], P(('dp', 'expert'))
The draws below stay inside these ranges and needn't reach their ends.
Inputs may be any that keep to these rules, and one draw needn't show every extreme that they name: `routes`: each row names 8 different experts. In the rows of one device (aligned blocks of 4 rows) no expert is named by more than 2 rows, a bound that some block reaches.
All inputs are finite; a program needn't handle non-finite values.
Results may differ from the reference program's by a relative error of at most 0.0098.
Values may be sent and summed in bfloat16 or wider, within the bound.
No kernel may reach another device: no remote copies, remote signals or barrier semaphores. Data moves between devices by JAX's collectives and lax.ppermute only.
A program may use at most 128 MiB of HBM per device.

```python
import math
import jax
import jax.numpy as jnp
import numpy as np
from jax import lax

D = 7168
FF = 2048
TOK_DEV = 4
EXPERTS = 32
TOP = 8
CAP = 2
TOKENS = 1024
N_DP = 8
N_EXPERT = 32


def level_of(rng, shape, shards, least, top_value):
    loudness, own = 1.0, jax.random.fold_in(rng, 6)
    for axis_at, shards_of in shards:
        heights = jnp.exp(jax.random.uniform(jax.random.fold_in(own, axis_at), (shards_of,), jnp.float32, least / len(shards), top_value / len(shards)))
        loudness = loudness * jnp.repeat(heights, shape[axis_at] // shards_of).reshape([-1 if axis == axis_at else 1 for axis in range(len(shape))])
    return loudness


def assign_block(stream_key, own, number, rows, amount, top, limit, lean):
    ranking = jax.random.permutation(stream_key, amount)
    crowded, usual = portions_of(amount, rows * top, limit, lean, True), portions_of(amount, rows * top, limit, lean, False)
    places = jnp.arange(amount)

    def named(tallies, rotation):
        used = int((tallies > 0).sum())
        fixed = max(1, used // 4)
        passed = fixed + (places - fixed + rotation * (used - fixed)) % max(1, amount - fixed)
        return jnp.zeros((amount,), jnp.int32).at[ranking[jnp.where(places < fixed, places, passed)]].set(jnp.asarray(tallies, jnp.int32))

    tallies = jnp.where(number % 4 == 0, named(crowded, number // 4), named(usual, number - number // 4 - 1))
    mixed = jax.random.permutation(jax.random.fold_in(own, 3), amount)
    donor, receiver = mixed[0:amount // 2 * 2:2], mixed[1:amount // 2 * 2:2]
    slack = jnp.minimum(tallies[donor] - 1, limit - tallies[receiver]) // 2
    slack = jnp.where((donor == ranking[0]) | (receiver == ranking[0]) | (tallies[receiver] == 0), 0, jnp.maximum(slack, 0))
    passed = jax.random.randint(jax.random.fold_in(own, 4), (amount // 2,), 0, 1 << 20) % (slack + 1)
    tallies = tallies.at[donor].add(-passed).at[receiver].add(passed)
    items = jnp.searchsorted(jnp.cumsum(tallies), jnp.arange(rows * top), side="right").astype(jnp.int32)
    listing = items.reshape(top, rows).T
    listing = listing[jax.random.permutation(jax.random.fold_in(own, 1), rows)]
    rotation = jax.random.randint(jax.random.fold_in(own, 2), (rows, 1), 0, top)
    return jnp.take_along_axis(listing, (jnp.arange(top)[None, :] + rotation) % top, axis=1)


def portions_of(amount, total, most, lean, full):
    weights = [(1 << 20) // math.isqrt(standing ** lean) + 1 for standing in range(1, amount + 1)]
    largest = most if full else min(most, max(-(-total // amount), total * weights[0] // sum(weights)))
    least = 1 if total - largest >= amount - 1 else 0
    counts, rest = [largest] + [least] * (amount - 1), total - largest - least * (amount - 1)
    while rest > 0:
        free = [i for i in range(1, amount) if counts[i] < largest] or [i for i in range(1, amount) if counts[i] < most]
        mass, left = sum([weights[i] for i in free]), rest
        for i in free:
            extra = min(most - counts[i], max(1, left * weights[i] // mass), rest)
            counts[i] = counts[i] + extra
            rest = rest - extra
    return np.array(counts)


def scatter_about(rng, extent, width, reach, cuts=(), kind=jnp.bfloat16):
    gain = level_of(rng, extent, cuts, -0.22, 0.18) if cuts else 1.0
    values = jax.random.normal(rng, extent, jnp.float32) * width * gain
    return jnp.minimum(jnp.maximum(values, -reach), reach).astype(kind)


def setup_inputs(seed: int = 0) -> dict:
    keys = jax.random.split(jax.random.key(seed), 7)
    tokens = scatter_about(keys[0], (TOKENS, D), 1.0, 6.0, ((0, 256),))
    routes_keys = jax.random.split(jax.random.fold_in(keys[1], 1), TOKENS // TOK_DEV)
    routes_turns = jax.random.permutation(jax.random.fold_in(keys[1], 3), TOKENS // TOK_DEV)
    routes = jax.vmap(lambda own, number: assign_block(jax.random.fold_in(keys[1], 2), own, number, TOK_DEV, EXPERTS, TOP, CAP, 2))(routes_keys, routes_turns).reshape((TOKENS, TOP))
    gate_scores = jnp.clip(jnp.exp(math.log(1.0) - 2.3025851 * jax.random.uniform(keys[2], (TOKENS, TOP), jnp.float32) ** level_of(keys[2], (TOKENS, TOP), ((0, 256),), -0.2, 0.2)), 0.1, 1.0)
    w_gate = scatter_about(keys[3], (EXPERTS, D, FF), D ** -0.5, 0.0625, ((0, 32), (2, 8)))
    w_up = scatter_about(keys[4], (EXPERTS, D, FF), D ** -0.5, 0.0625, ((0, 32), (2, 8)))
    w_down = scatter_about(keys[5], (EXPERTS, FF, D), FF ** -0.5, 0.125, ((0, 32), (1, 8)))
    return dict(tokens=tokens, routes=routes, gate_scores=gate_scores, w_gate=w_gate, w_up=w_up, w_down=w_down)


def reference(tokens, routes, gate_scores, w_gate, w_up, w_down):
    token_count = tokens.shape[0]
    row_limit = min(token_count, N_DP * N_EXPERT * CAP)

    def one_expert(totals, inputs):
        expert_id, gate_mat, up_mat, down_mat = inputs
        matched = routes == expert_id
        chosen = jnp.any(matched, axis=1).astype(jnp.int32)
        route_weight = jnp.sum(jnp.where(matched, gate_scores, 0.0), axis=1)
        ranked = jnp.argsort(1 - chosen, stable=True)[:row_limit].astype(jnp.int32)
        picked_rows = tokens[ranked]
        gate_act = jnp.dot(picked_rows, gate_mat, preferred_element_type=jnp.float32)
        up_act = jnp.dot(picked_rows, up_mat, preferred_element_type=jnp.float32)
        hidden = (jax.nn.silu(gate_act) * up_act).astype(jnp.bfloat16)
        expert_out = jnp.dot(hidden, down_mat, preferred_element_type=jnp.float32)
        totals = totals.at[ranked].add(expert_out * route_weight[ranked][:, None])
        return totals, None

    numbers = jnp.arange(w_gate.shape[0], dtype=jnp.int32)
    start_sum = jnp.zeros(tokens.shape, jnp.float32)
    totals, _ = lax.scan(one_expert, start_sum, (numbers, w_gate, w_up, w_down))
    return totals.astype(jnp.bfloat16)
```

```python
import functools

import jax
import jax.numpy as jnp
from jax import lax
from jax.experimental import pallas as pl
from jax.experimental.pallas import tpu as pltpu
from jax.sharding import Mesh, PartitionSpec as P


LANES = 128
ORDER = (2, 1, 3, 0)


def shift(value, axis, step):
    n = lax.axis_size(axis)
    return lax.ppermute(value, axis, [(i, (i + step) % n) for i in range(n)])


def ring_gather(own, axis):
    half = own.shape[0] // 2
    prev = shift(own, axis, 1)
    succ = shift(own, axis, -1)
    low = shift(prev[:half], axis, 1)
    high = shift(succ[half:], axis, -1)
    return own, succ, low, high, prev


def ring_reduce(own, succ, low, high, prev, axis):
    half = low.shape[0]
    got_low = shift(low, axis, 1)
    got_high = shift(high, axis, -1)
    to_succ = jnp.concatenate([added(succ[:half], got_low), succ[half:]], axis=0)
    to_prev = jnp.concatenate([prev[:half], added(prev[half:], got_high)], axis=0)
    return added(own, shift(to_succ, axis, 1), shift(to_prev, axis, -1))


def added(*terms):
    total = terms[0].astype(jnp.float32)
    for term in terms[1:]:
        total = total + term.astype(jnp.float32)
    return total.astype(jnp.bfloat16)


def by_core(core, if_zero, if_one):
    return jnp.where(core == 0, if_zero, if_one)


def hidden_kernel(widths, place_ref, *refs):
    pieces, (gate_ref, up_ref, out_ref), scratch = refs[:20], refs[20:23], refs[23:]
    bufs, w_buf, acc, x_sem, w_sem = scratch[:20], scratch[20], scratch[21], scratch[22], scratch[23]
    half_rows = w_buf.shape[1]
    ff = gate_ref.shape[1]
    core, expert = place_ref[0], place_ref[1]
    copies = []
    for side in range(2):
        which = core if side == 0 else 1 - core
        rows = pl.ds(pl.multiple_of(which * half_rows, LANES), half_rows)
        for k, ref in enumerate((gate_ref, up_ref)):
            copies.append(
                pltpu.make_async_copy(
                    ref.at[rows, :], w_buf.at[side, :, k * ff : (k + 1) * ff], w_sem.at[side, k]
                )
            )
    x_copies = [pltpu.make_async_copy(p, b, x_sem.at[i]) for i, (p, b) in enumerate(zip(pieces, bufs))]
    for c in copies[:2] + x_copies[:10] + copies[2:] + x_copies[10:]:
        c.start()
    for side in range(2):
        copies[2 * side].wait()
        copies[2 * side + 1].wait()
        start = 0
        for colour in range(2):
            skip = LANES if colour == 0 else 0
            width = widths[colour]
            for k in range(5):
                i = side * 10 + colour * 5 + k
                x_copies[i].wait()
                buf = bufs[i]
                count = buf.shape[0]
                x = buf[:, :, skip : skip + width].reshape(count * buf.shape[1], width)
                part = jnp.dot(
                    x, w_buf[side, start : start + width, :], preferred_element_type=jnp.float32
                ).reshape(count, buf.shape[1], 2 * ff)
                offset, first = ((0, 0), (1, 0), (2, 0), (2, 2), (3, 0))[k]
                for j in range(count):
                    at = (offset, first + j) if colour == 0 else (first + j, offset)
                    if side == 0 and colour == 0:
                        acc[at[0], at[1]] = part[j]
                    else:
                        acc[at[0], at[1]] += part[j]
            start += width
    lane = lax.broadcasted_iota(jnp.int32, (LANES, ff), 0)
    chosen = ((lane == expert) | (lane == expert + LANES // 2)).astype(jnp.bfloat16)
    for k in range(5):
        buf = bufs[k]
        offset, first = ((0, 0), (1, 0), (2, 0), (2, 2), (3, 0))[k]
        for j in range(buf.shape[0]):
            weight = jnp.dot(buf[j, :, :LANES], chosen, preferred_element_type=jnp.float32)
            gate = acc[offset, first + j, :, :ff]
            up = acc[offset, first + j, :, ff:]
            act = gate / (1.0 + jnp.exp(-gate)) * up * weight
            out_ref[offset, first + j] = act.astype(jnp.bfloat16)


def hidden_call(place, own, sibling, gate_mat, up_mat, widths):
    rows = own[0].shape[1]
    ff = gate_mat.shape[1]
    pieces = (*own, *sibling)
    any_spec = pl.BlockSpec(memory_space=pl.ANY)
    flops = 2 * 16 * rows * gate_mat.shape[0] * 2 * ff
    return pl.pallas_call(
        functools.partial(hidden_kernel, widths),
        out_shape=jax.ShapeDtypeStruct((4, 4, rows, ff), jnp.bfloat16),
        in_specs=[pl.BlockSpec(memory_space=pltpu.SMEM)] + [any_spec] * 22,
        out_specs=pl.BlockSpec(memory_space=pltpu.VMEM),
        scratch_shapes=[pltpu.VMEM(p.shape, p.dtype) for p in pieces]
        + [
            pltpu.VMEM((2, gate_mat.shape[0] // 2, 2 * ff), jnp.bfloat16),
            pltpu.VMEM((4, 4, rows, 2 * ff), jnp.float32),
            pltpu.SemaphoreType.DMA((20,)),
            pltpu.SemaphoreType.DMA((2, 2)),
        ],
        compiler_params=pltpu.CompilerParams(vmem_limit_bytes=40 * 2**20),
        cost_estimate=pl.CostEstimate(flops=flops, bytes_accessed=24 * 2**20, transcendentals=0),
        name="hidden",
    )(place, *pieces, gate_mat, up_mat)


def down_kernel(colour, adds, place_ref, h_ref, w_ref, *refs):
    recv_ref = refs[0] if adds else None
    refs = refs[1:] if adds else refs
    n_out = 5 if adds else 1
    outs, (w_buf, o_buf, *r_buf), (w_sem, o_sem, r_sem) = refs[:n_out], refs[n_out:-3], refs[-3:]
    ff, width = w_buf.shape
    half = place_ref[0] if adds else 1 - place_ref[0]
    columns = pl.ds(pl.multiple_of((half * 2 + colour) * width, LANES), width)
    w_copy = pltpu.make_async_copy(w_ref.at[:, columns], w_buf, w_sem)
    w_copy.start()
    r_copies = []
    if adds:
        for offset in range(4):
            r_copies.append(
                pltpu.make_async_copy(recv_ref.at[offset], r_buf[0].at[offset], r_sem.at[offset])
            )
        for offset in ORDER:
            r_copies[offset].start()
    w_copy.wait()
    tile = 2 * LANES if width % (2 * LANES) == 0 else LANES
    o_copies = []
    for offset in ORDER:
        h = h_ref[offset] if colour == 0 else h_ref[:, offset]
        h = h.reshape(-1, ff)
        if adds:
            r_copies[offset].wait()
        for at in range(0, width, tile):
            part = jnp.dot(h, w_buf[:, at : at + tile], preferred_element_type=jnp.float32)
            part = part.reshape(4, -1, tile)
            if adds:
                part = part + r_buf[0][offset, :, :, at : at + tile].astype(jnp.float32)
            o_buf[offset, :, :, at : at + tile] = part.astype(jnp.bfloat16)
        if not adds:
            todo = [(o_buf.at[offset], outs[0].at[offset])]
        elif offset == 2:
            todo = [(o_buf.at[2, 0:2], outs[2]), (o_buf.at[2, 2:4], outs[3])]
        else:
            todo = [(o_buf.at[offset], outs[{0: 0, 1: 1, 3: 4}[offset]])]
        for source, target in todo:
            copy = pltpu.make_async_copy(source, target, o_sem.at[len(o_copies)])
            copy.start()
            o_copies.append(copy)
    for copy in o_copies:
        copy.wait()


def down_call(place, hidden, down_mat, colour, received):
    adds = received is not None
    rows, ff = hidden.shape[2:]
    width = down_mat.shape[1] // 4
    any_spec = pl.BlockSpec(memory_space=pl.ANY)

    def piece(*lead):
        return jax.ShapeDtypeStruct((*lead, rows, width), jnp.bfloat16)

    whole = pltpu.VMEM((4, 4, rows, width), jnp.bfloat16)
    return pl.pallas_call(
        functools.partial(down_kernel, colour, adds),
        out_shape=[piece(4), piece(4), piece(2), piece(2), piece(4)] if adds else [piece(4, 4)],
        in_specs=[
            pl.BlockSpec(memory_space=pltpu.SMEM),
            pl.BlockSpec(memory_space=pltpu.VMEM),
            any_spec,
        ]
        + [any_spec] * adds,
        out_specs=[any_spec] * (5 if adds else 1),
        scratch_shapes=[pltpu.VMEM((ff, width), jnp.bfloat16), whole]
        + [whole] * adds
        + [
            pltpu.SemaphoreType.DMA,
            pltpu.SemaphoreType.DMA((5,)),
            pltpu.SemaphoreType.DMA((4,)),
        ],
        compiler_params=pltpu.CompilerParams(vmem_limit_bytes=20 * 2**20),
        cost_estimate=pl.CostEstimate(
            flops=2 * 16 * rows * ff * width,
            bytes_accessed=2 * 16 * rows * width * (2 if adds else 1),
            transcendentals=0,
        ),
        name="down",
    )(place, hidden, down_mat, *([received] if adds else []))


def shards(tokens, routes, gate_scores, w_gate, w_up, w_down):
    tok_rows, model_width = tokens.shape
    half = model_width // 2
    core = lax.axis_index("c")
    expert = lax.axis_index(("y", "x", "c")).astype(jnp.int32)
    place = jnp.stack([core.astype(jnp.int32), expert])

    experts = lax.axis_size(("y", "x", "c"))
    named = routes[:, :, None] == jnp.arange(experts, dtype=jnp.int32)
    weights = jnp.sum(jnp.where(named, gate_scores[:, :, None], 0.0), axis=1)
    top = lax.reduce_precision(weights, 8, 7)
    pad = jnp.zeros((tok_rows, LANES // 2 - experts), jnp.float32)
    tile = jnp.concatenate([top, pad, weights - top, pad], axis=1).astype(jnp.bfloat16)

    first, second = tokens[:, :half], tokens[:, half:]
    mine = jnp.concatenate([tile, by_core(core, first, second)], axis=1)
    theirs = jnp.concatenate([tile, by_core(core, second, first)], axis=1)
    other = shift(theirs, "c", 1)
    block = by_core(
        core, jnp.concatenate([mine, other], axis=0), jnp.concatenate([other, mine], axis=0)
    )

    n_z = lax.axis_size("z")
    column = jnp.stack([block] + [shift(block, "z", -k) for k in range(1, n_z)])
    column = column.reshape(-1, column.shape[-1])
    cut = LANES + half // 2
    gathered = []
    for part, (near, far) in ((column[:, :cut], ("x", "y")), (column[:, cut:], ("y", "x"))):
        own, succ, low, high, prev = ring_gather(part, near)
        line = jnp.stack([own, succ, jnp.concatenate([low, high], axis=0), prev])
        gathered.extend(ring_gather(line, far))
    swapped = [shift(piece, "c", 1) for piece in gathered]

    widths = (half // 2, half // 2)
    hidden = hidden_call(place, gathered, swapped, w_gate[0], w_up[0], widths)

    down_mat = w_down[0]
    sent = [down_call(place, hidden, down_mat, colour, None)[0] for colour in range(2)]
    received = [shift(value, "c", 1) for value in sent]
    sums = []
    for colour, (near, far) in enumerate((("x", "y"), ("y", "x"))):
        pieces = down_call(place, hidden, down_mat, colour, received[colour])
        line = ring_reduce(*pieces, far)
        cut = line.shape[1] // 2
        sums.append(ring_reduce(line[0], line[1], line[2, :cut], line[2, cut:], line[3], near))
    column = jnp.concatenate(sums, axis=1).reshape(n_z, -1, half)
    total = added(column[0], *[shift(column[k], "z", k) for k in range(1, n_z)])

    mine = by_core(core, total[:tok_rows], total[tok_rows:])
    theirs = by_core(core, total[tok_rows:], total[:tok_rows])
    other = shift(theirs, "c", 1)
    return by_core(
        core, jnp.concatenate([mine, other], axis=1), jnp.concatenate([other, mine], axis=1)
    )


def solution(mesh):
    grid = Mesh(mesh.devices.reshape(8, 4, 4, 2), ("z", "y", "x", "c"))
    every = ("z", "y", "x", "c")
    plane = ("y", "x", "c")
    return jax.shard_map(
        shards,
        mesh=grid,
        in_specs=(
            P(every, None),
            P(every, None),
            P(every, None),
            P(plane, None, "z"),
            P(plane, None, "z"),
            P(plane, "z", None),
        ),
        out_specs=P(every, None),
        check_vma=False,
    )
```

```python
import functools

import jax
import jax.numpy as jnp
from jax import lax
from jax.experimental import pallas as pl
from jax.experimental.pallas import tpu as pltpu
from jax.sharding import Mesh, PartitionSpec as P


LANES = 128


def shift(value, axis, step):
    n = lax.axis_size(axis)
    return lax.ppermute(value, axis, [(i, (i + step) % n) for i in range(n)])


def near_gather(own, axis):
    return jnp.stack([own, shift(own, axis, -1), shift(own, axis, 2), shift(own, axis, 1)])


def near_reduce(own, succ, across, prev, axis):
    return added(own, shift(succ, axis, 1), shift(across, axis, 2), shift(prev, axis, -1))


def far_gather(own, axis):
    half = own.shape[0] // 2
    prev = shift(own, axis, 1)
    succ = shift(own, axis, -1)
    low = shift(prev[:half], axis, 1)
    high = shift(succ[half:], axis, -1)
    return own, succ, low, high, prev


def far_reduce(own, succ, low, high, prev, axis):
    half = low.shape[0]
    got_low = shift(low, axis, 1)
    got_high = shift(high, axis, -1)
    to_succ = jnp.concatenate([added(succ[:half], got_low), succ[half:]], axis=0)
    to_prev = jnp.concatenate([prev[:half], added(prev[half:], got_high)], axis=0)
    return added(own, shift(to_succ, axis, 1), shift(to_prev, axis, -1))


def added(*terms):
    total = terms[0].astype(jnp.float32)
    for term in terms[1:]:
        total = total + term.astype(jnp.float32)
    return total.astype(jnp.bfloat16)


def by_core(core, if_zero, if_one):
    return jnp.where(core == 0, if_zero, if_one)


PLACES = ((0, 0, 4), (1, 0, 4), (2, 0, 2), (2, 2, 2), (3, 0, 4))


def hidden_kernel(place_ref, *refs):
    pieces, (gate_ref, up_ref, out_ref) = refs[:20], refs[20:23]
    x_buf, w_buf, acc, named, x_sem, w_sem, named_sem = refs[23:]
    rows, width = x_buf.shape[3:]
    ff = gate_ref.shape[1]
    core, expert = place_ref[0], place_ref[1]
    for side in range(2):
        which = core if side == 0 else 1 - core
        half = pl.ds(pl.multiple_of(which * 2 * width, LANES), 2 * width)
        for k, ref in enumerate((gate_ref, up_ref)):
            pltpu.make_async_copy(
                ref.at[half, :], w_buf.at[side, :, k * ff : (k + 1) * ff], w_sem.at[side]
            ).start()
        for i in range(side * 10, side * 10 + 10):
            group = i // 5
            offset, first, count = PLACES[i % 5]
            skip = pieces[i].shape[2] - width
            pltpu.make_async_copy(
                pieces[i].at[:, :, skip : skip + width],
                x_buf.at[group, offset, first : first + count],
                x_sem.at[group, offset],
            ).start()
    for i, (offset, first, count) in enumerate(PLACES):
        pltpu.make_async_copy(
            pieces[i].at[:, :, :LANES], named.at[offset, first : first + count], named_sem
        ).start()

    def step(i, _):
        group, offset = i // 4, i % 4
        side, colour = group // 2, group % 2

        @pl.when(i % 8 == 0)
        def _():
            pltpu.make_async_copy(w_buf.at[side], w_buf.at[side], w_sem.at[side]).wait()

        there = x_buf.at[group, offset]
        pltpu.make_async_copy(there, there, x_sem.at[group, offset]).wait()
        x = x_buf[group, offset].reshape(4 * rows, width)
        w = w_buf[side, pl.ds(pl.multiple_of(colour * width, LANES), width), :]
        part = jnp.dot(x, w, preferred_element_type=jnp.float32).reshape(4, rows, 2 * ff)
        acc[colour, offset] = jnp.where(side == 0, part, part + acc[colour, offset])
        return 0

    lax.fori_loop(0, 16, step, 0)
    pltpu.make_async_copy(named, named, named_sem).wait()
    lane = lax.broadcasted_iota(jnp.int32, (LANES, ff), 0)
    chosen = ((lane == expert) | (lane == expert + LANES // 2)).astype(jnp.bfloat16)

    def finish(offset, _):
        weight = jnp.dot(
            named[offset].reshape(4 * rows, LANES), chosen, preferred_element_type=jnp.float32
        ).reshape(4, rows, ff)
        for j in range(4):
            gate = acc[0, offset, j, :, :ff] + acc[1, j, offset, :, :ff]
            up = acc[0, offset, j, :, ff:] + acc[1, j, offset, :, ff:]
            act = (gate / (1.0 + jnp.exp(-gate)) * up * weight[j]).astype(jnp.bfloat16)
            out_ref[0, offset, j] = act
            out_ref[1, j, offset] = act
        return 0

    lax.fori_loop(0, 4, finish, 0)


def hidden_call(place, own, sibling, gate_mat, up_mat):
    rows = own[0].shape[1]
    ff = gate_mat.shape[1]
    width = gate_mat.shape[0] // 4
    any_spec = pl.BlockSpec(memory_space=pl.ANY)
    return pl.pallas_call(
        hidden_kernel,
        out_shape=jax.ShapeDtypeStruct((2, 4, 4, rows, ff), jnp.bfloat16),
        in_specs=[pl.BlockSpec(memory_space=pltpu.SMEM)] + [any_spec] * 22,
        out_specs=pl.BlockSpec(memory_space=pltpu.VMEM),
        scratch_shapes=[
            pltpu.VMEM((4, 4, 4, rows, width), jnp.bfloat16),
            pltpu.VMEM((2, 2 * width, 2 * ff), jnp.bfloat16),
            pltpu.VMEM((2, 4, 4, rows, 2 * ff), jnp.float32),
            pltpu.VMEM((4, 4, rows, LANES), jnp.bfloat16),
            pltpu.SemaphoreType.DMA((4, 4)),
            pltpu.SemaphoreType.DMA((2,)),
            pltpu.SemaphoreType.DMA,
        ],
        compiler_params=pltpu.CompilerParams(vmem_limit_bytes=40 * 2**20),
        cost_estimate=pl.CostEstimate(
            flops=2 * 16 * rows * gate_mat.shape[0] * 2 * ff,
            bytes_accessed=24 * 2**20,
            transcendentals=0,
        ),
        name="hidden",
    )(place, *own, *sibling, gate_mat, up_mat)


def down_kernel(offsets, adds, place_ref, h_ref, w_ref, *refs):
    recv_ref = refs[0] if adds else None
    refs = refs[1:] if adds else refs
    count = len(offsets)
    n_out = len(refs) - 6 if adds else 1
    outs = refs[:n_out]
    w_buf, o_buf, *r_buf, w_sem, o_sem, r_sem = refs[n_out:]
    ff, width = w_buf.shape[1:]
    half = place_ref[0] if adds else 1 - place_ref[0]
    for colour in range(2):
        columns = pl.ds(pl.multiple_of((half * 2 + colour) * width, LANES), width)
        pltpu.make_async_copy(w_ref.at[:, columns], w_buf.at[colour], w_sem.at[colour]).start()
    units = [(k, colour) for k in range(count) for colour in range(2)]
    for k, colour in units if adds else ():
        pltpu.make_async_copy(recv_ref.at[k, colour], r_buf[0].at[k, colour], r_sem.at[k, colour]).start()
    steps = 2 if width % (4 * LANES) == 0 else 1
    tile = width // steps

    def copies(i):
        k, colour = units[i]
        if not adds:
            todo = [(o_buf.at[k, colour], outs[0].at[k, colour])]
        else:
            each, length = n_out // len(units), outs[0].shape[0]
            todo = [
                (o_buf.at[k, colour, length * j : length * (j + 1)], outs[i * each + j])
                for j in range(each)
            ]
        return [pltpu.make_async_copy(a, b, o_sem.at[i, j]) for j, (a, b) in enumerate(todo)]

    def unit(i, _):
        k, colour = i // 2, i % 2
        offset = k + k // 2 if count > 1 else offsets[0]

        @pl.when(k == 0)
        def _():
            pltpu.make_async_copy(w_buf.at[colour], w_buf.at[colour], w_sem.at[colour]).wait()

        if adds:
            there = r_buf[0].at[k, colour]
            pltpu.make_async_copy(there, there, r_sem.at[k, colour]).wait()
        h = h_ref[colour, offset].reshape(-1, ff)

        def column(t, _):
            at = pl.ds(pl.multiple_of(t * tile, LANES), tile)
            part = jnp.dot(h, w_buf[colour, :, at], preferred_element_type=jnp.float32)
            part = part.reshape(4, -1, tile)
            if adds:
                part = part + r_buf[0][k, colour, :, :, at].astype(jnp.float32)
            o_buf[k, colour, :, :, at] = part.astype(jnp.bfloat16)
            return 0

        lax.fori_loop(0, steps, column, 0)
        for u in range(2 * count):

            @pl.when(i == u)
            def _(u=u):
                for copy in copies(u):
                    copy.start()

        return 0

    lax.fori_loop(0, 2 * count, unit, 0)
    for u in range(2 * count):
        for copy in copies(u):
            copy.wait()


def down_call(place, hidden, down_mat, offsets, received):
    adds = received is not None
    rows, ff = hidden.shape[3:]
    width = down_mat.shape[1] // 4
    count = len(offsets)
    any_spec = pl.BlockSpec(memory_space=pl.ANY)
    whole = (count, 2, 4, rows, width)
    parts = 2 if offsets == (2,) else 1
    piece = jax.ShapeDtypeStruct((4 // parts, rows, width), jnp.bfloat16)
    moved = 2 * 2 * count * 4 * rows * width
    return pl.pallas_call(
        functools.partial(down_kernel, offsets, adds),
        out_shape=[piece] * (2 * count * parts) if adds else [jax.ShapeDtypeStruct(whole, jnp.bfloat16)],
        in_specs=[
            pl.BlockSpec(memory_space=pltpu.SMEM),
            pl.BlockSpec(memory_space=pltpu.VMEM),
            any_spec,
        ]
        + [any_spec] * adds,
        out_specs=[any_spec] * (2 * count * parts if adds else 1),
        scratch_shapes=[pltpu.VMEM((2, ff, width), jnp.bfloat16)]
        + [pltpu.VMEM(whole, jnp.bfloat16)] * (1 + adds)
        + [
            pltpu.SemaphoreType.DMA((2,)),
            pltpu.SemaphoreType.DMA((2 * count, 2)),
            pltpu.SemaphoreType.DMA((count, 2)),
        ],
        compiler_params=pltpu.CompilerParams(vmem_limit_bytes=20 * 2**20),
        cost_estimate=pl.CostEstimate(
            flops=2 * count * 8 * rows * ff * width,
            bytes_accessed=moved * (2 if adds else 1),
            transcendentals=0,
        ),
        name="down_add" if adds else "down_send",
    )(place, hidden, down_mat, *([received] if adds else []))


def step(tokens, routes, gate_scores, w_gate, w_up, w_down):
    tok_rows, model_width = tokens.shape
    half = model_width // 2
    core = lax.axis_index("c")
    expert = lax.axis_index(("y", "x", "c")).astype(jnp.int32)
    place = jnp.stack([core.astype(jnp.int32), expert])

    experts = lax.axis_size(("y", "x", "c"))
    named = routes[:, :, None] == jnp.arange(experts, dtype=jnp.int32)
    weights = jnp.sum(jnp.where(named, gate_scores[:, :, None], 0.0), axis=1)
    top = lax.reduce_precision(weights, 8, 7)
    pad = jnp.zeros((tok_rows, LANES // 2 - experts), jnp.float32)
    tile = jnp.concatenate([top, pad, weights - top, pad], axis=1).astype(jnp.bfloat16)

    first, second = tokens[:, :half], tokens[:, half:]
    mine = jnp.concatenate([tile, by_core(core, first, second)], axis=1)
    theirs = jnp.concatenate([tile, by_core(core, second, first)], axis=1)
    other = shift(theirs, "c", 1)
    block = by_core(
        core, jnp.concatenate([mine, other], axis=0), jnp.concatenate([other, mine], axis=0)
    )

    n_z = lax.axis_size("z")
    column = jnp.broadcast_to(block, (n_z, *block.shape))
    column = lax.all_to_all(column, "z", split_axis=0, concat_axis=0, tiled=True)
    column = column.reshape(-1, block.shape[1])
    cut = LANES + half // 2
    gathered = []
    for part, (near, far) in ((column[:, :cut], ("x", "y")), (column[:, cut:], ("y", "x"))):
        gathered.extend(far_gather(near_gather(part, near), far))
    swapped = [shift(piece, "c", 1) for piece in gathered]
    hidden = hidden_call(place, gathered, swapped, w_gate[0], w_up[0])

    down_mat = w_down[0]
    groups = ((2,), (0, 1, 3))
    far_sent = down_call(place, hidden, down_mat, groups[0], None)[0]
    far_got = shift(far_sent, "c", 1)
    sent = down_call(place, hidden, down_mat, groups[1], None)[0]
    across = down_call(place, hidden, down_mat, groups[0], far_got)
    got = shift(sent, "c", 1)
    others = down_call(place, hidden, down_mat, groups[1], got)
    sums = []
    for colour, (near, far) in enumerate((("x", "y"), ("y", "x"))):
        own, succ, prev = others[colour::2]
        low, high = across[2 * colour : 2 * colour + 2]
        line = far_reduce(own, succ, low, high, prev, far)
        sums.append(near_reduce(line[0], line[1], line[2], line[3], near))
    column = jnp.concatenate(sums, axis=1).reshape(n_z, -1, half)
    column = lax.all_to_all(column, "z", split_axis=0, concat_axis=0, tiled=True)
    total = added(*[column[k] for k in range(n_z)])

    mine = by_core(core, total[:tok_rows], total[tok_rows:])
    theirs = by_core(core, total[tok_rows:], total[:tok_rows])
    other = shift(theirs, "c", 1)
    return by_core(
        core, jnp.concatenate([mine, other], axis=1), jnp.concatenate([other, mine], axis=1)
    )


def solution(mesh):
    grid = Mesh(mesh.devices.reshape(8, 4, 4, 2), ("z", "y", "x", "c"))
    every = ("z", "y", "x", "c")
    plane = ("y", "x", "c")
    return jax.shard_map(
        step,
        mesh=grid,
        in_specs=(
            P(every, None),
            P(every, None),
            P(every, None),
            P(plane, None, "z"),
            P(plane, None, "z"),
            P(plane, "z", None),
        ),
        out_specs=P(every, None),
        check_vma=False,
    )
```

```python
import functools

import jax
import jax.numpy as jnp
from jax import lax
from jax.experimental import pallas as pl
from jax.experimental.pallas import tpu as pltpu
from jax.sharding import Mesh, PartitionSpec as P


LANES = 128


def shift(value, axis, step):
    n = lax.axis_size(axis)
    return lax.ppermute(value, axis, [(i, (i + step) % n) for i in range(n)])


def near_gather(own, axis):
    return jnp.concatenate([own, shift(own, axis, -1), shift(own, axis, 2), shift(own, axis, 1)])


def near_reduce(own, succ, across, prev, axis):
    return added(own, shift(succ, axis, 1), shift(across, axis, 2), shift(prev, axis, -1))


def far_gather(own, axis):
    n = lax.axis_size(axis)
    half = own.shape[0] // 2
    pieces = [(0, 0, own)]
    prev = succ = own
    for k in range(1, n // 2):
        prev, succ = shift(prev, axis, 1), shift(succ, axis, -1)
        pieces += [(k, 0, succ), (n - k, 0, prev)]
    low, high = shift(prev[:half], axis, 1), shift(succ[half:], axis, -1)
    return pieces + [(n // 2, 0, low), (n // 2, half, high)]


def far_reduce(own, succ, low, high, prev, axis):
    half = low.shape[0]
    got_low = shift(low, axis, 1)
    got_high = shift(high, axis, -1)
    to_succ = jnp.concatenate([added(succ[:half], got_low), succ[half:]], axis=0)
    to_prev = jnp.concatenate([prev[:half], added(prev[half:], got_high)], axis=0)
    return added(own, shift(to_succ, axis, 1), shift(to_prev, axis, -1))


def added(*terms):
    total = terms[0].astype(jnp.float32)
    for term in terms[1:]:
        total = total + term.astype(jnp.float32)
    return total.astype(jnp.bfloat16)


def by_core(core, if_zero, if_one):
    return jnp.where(core == 0, if_zero, if_one)


def hidden_kernel(count, spots, place_ref, *refs):
    sources, (gate_ref, up_ref, down_ref, out_ref, sent_ref) = refs[:count], refs[count : count + 5]
    x_buf, w_buf, acc, named, d_buf, o_buf, x_sem, w_sem, named_sem, d_sem, o_sem = refs[count + 5 :]
    lines, width = x_buf.shape[2:]
    rows = lines // 4
    ff = gate_ref.shape[1]
    core, expert = place_ref[0], place_ref[1]
    for side in range(2):
        half = core if side == 0 else 1 - core
        for colour in range(2):
            part = pl.ds(pl.multiple_of((2 * half + colour) * width, LANES), width)
            for k, ref in enumerate((gate_ref, up_ref)):
                pltpu.make_async_copy(
                    ref.at[part, :],
                    w_buf.at[2 * side + colour, :, k * ff : (k + 1) * ff],
                    w_sem.at[2 * side + colour],
                ).start()
        for which, colour, first, source, begin, length in spots:
            if which == side:
                skip = sources[source].shape[1] - width
                block, row = first // lines, first % lines
                pltpu.make_async_copy(
                    sources[source].at[begin : begin + length, skip : skip + width],
                    x_buf.at[2 * side + colour, block, row : row + length],
                    x_sem.at[2 * side + colour, block],
                ).start()
    for side, colour, first, source, begin, length in spots:
        if side == 0 and colour == 0:
            pltpu.make_async_copy(
                sources[source].at[begin : begin + length, :LANES],
                named.at[first // lines, first % lines : first % lines + length],
                named_sem,
            ).start()

    for colour in range(2):
        part = pl.ds(pl.multiple_of((2 * (1 - core) + colour) * width, LANES), width)
        pltpu.make_async_copy(down_ref.at[:, part], d_buf.at[colour], d_sem.at[colour]).start()

    def step(i, _):
        group, pair = i // 2, i % 2
        side, colour = group // 2, group % 2

        @pl.when(pair == 0)
        def _():
            pltpu.make_async_copy(w_buf.at[group], w_buf.at[group], w_sem.at[group]).wait()

        for block in range(2):
            there = x_buf.at[group, 2 * pair + block]
            pltpu.make_async_copy(there, there, x_sem.at[group, 2 * pair + block]).wait()
        x = x_buf[group, pl.ds(2 * pair, 2)].reshape(2 * lines, width)
        part = jnp.dot(x, w_buf[group], preferred_element_type=jnp.float32)
        at = pl.ds(pl.multiple_of(2 * pair * lines, 8), 2 * lines)
        acc[colour, at, :] = jnp.where(side == 0, part, part + acc[colour, at, :])
        return 0

    lax.fori_loop(0, 8, step, 0)
    pltpu.make_async_copy(named, named, named_sem).wait()
    lane = lax.broadcasted_iota(jnp.int32, (LANES, ff), 0)
    chosen = ((lane == expert) | (lane == expert + LANES // 2)).astype(jnp.bfloat16)

    def finish(offset, _):
        weight = jnp.dot(named[offset], chosen, preferred_element_type=jnp.float32)
        for j in range(4):
            theirs = pl.ds(pl.multiple_of(j * lines + offset * rows, 8), rows)
            mine = pl.ds(pl.multiple_of(offset * lines + j * rows, 8), rows)
            total = acc[0, mine, :] + acc[1, theirs, :]
            gate, up = total[:, :ff], total[:, ff:]
            act = gate / (1.0 + jnp.exp(-gate)) * up * weight[j * rows : (j + 1) * rows]
            act = act.astype(jnp.bfloat16)
            out_ref[0, offset, j] = act
            out_ref[1, j, offset] = act
        return 0

    lax.fori_loop(0, 4, finish, 0)

    steps = 2 if width % (4 * LANES) == 0 else 1
    tile = width // steps
    for colour in range(2):
        pltpu.make_async_copy(d_buf.at[colour], d_buf.at[colour], d_sem.at[colour]).wait()

    def column(i, _):
        colour = i // steps
        at = pl.ds(pl.multiple_of(i % steps * tile, LANES), tile)
        h = out_ref[colour, 2].reshape(lines, ff)
        part = jnp.dot(h, d_buf[colour, :, at], preferred_element_type=jnp.float32)
        o_buf[0, colour, :, :, at] = part.reshape(4, rows, tile).astype(jnp.bfloat16)
        return 0

    lax.fori_loop(0, 2 * steps, column, 0)
    copy = pltpu.make_async_copy(o_buf, sent_ref, o_sem)
    copy.start()
    copy.wait()


def hidden_call(place, spots, sources, gate_mat, up_mat, down_mat):
    lines = sources[0].shape[0]
    rows = lines // 4
    ff = gate_mat.shape[1]
    width = gate_mat.shape[0] // 4
    any_spec = pl.BlockSpec(memory_space=pl.ANY)
    return pl.pallas_call(
        functools.partial(hidden_kernel, len(sources), spots),
        out_shape=[
            jax.ShapeDtypeStruct((2, 4, 4, rows, ff), jnp.bfloat16),
            jax.ShapeDtypeStruct((1, 2, 4, rows, width), jnp.bfloat16),
        ],
        in_specs=[pl.BlockSpec(memory_space=pltpu.SMEM)] + [any_spec] * (len(sources) + 3),
        out_specs=[pl.BlockSpec(memory_space=pltpu.VMEM), any_spec],
        scratch_shapes=[
            pltpu.VMEM((4, 4, lines, width), jnp.bfloat16),
            pltpu.VMEM((4, width, 2 * ff), jnp.bfloat16),
            pltpu.VMEM((2, 4 * lines, 2 * ff), jnp.float32),
            pltpu.VMEM((4, lines, LANES), jnp.bfloat16),
            pltpu.VMEM((2, ff, width), jnp.bfloat16),
            pltpu.VMEM((1, 2, 4, rows, width), jnp.bfloat16),
            pltpu.SemaphoreType.DMA((4, 4)),
            pltpu.SemaphoreType.DMA((4,)),
            pltpu.SemaphoreType.DMA,
            pltpu.SemaphoreType.DMA((2,)),
            pltpu.SemaphoreType.DMA,
        ],
        compiler_params=pltpu.CompilerParams(vmem_limit_bytes=36 * 2**20),
        cost_estimate=pl.CostEstimate(
            flops=2 * 16 * rows * gate_mat.shape[0] * 2 * ff,
            bytes_accessed=24 * 2**20,
            transcendentals=0,
        ),
        name="hidden",
    )(place, *sources, gate_mat, up_mat, down_mat)


def down_kernel(offsets, adds, place_ref, h_ref, w_ref, *refs):
    recv_ref = refs[0] if adds else None
    refs = refs[1:] if adds else refs
    count = len(offsets)
    n_out = len(refs) - 6 if adds else 1
    outs = refs[:n_out]
    w_buf, o_buf, *r_buf, w_sem, o_sem, r_sem = refs[n_out:]
    ff, width = w_buf.shape[1:]
    half = place_ref[0] if adds else 1 - place_ref[0]
    for colour in range(2):
        columns = pl.ds(pl.multiple_of((half * 2 + colour) * width, LANES), width)
        pltpu.make_async_copy(w_ref.at[:, columns], w_buf.at[colour], w_sem.at[colour]).start()
    units = [(k, colour) for k in range(count) for colour in range(2)]
    for k, colour in units if adds else ():
        pltpu.make_async_copy(recv_ref.at[k, colour], r_buf[0].at[k, colour], r_sem.at[k, colour]).start()
    steps = 2 if width % (4 * LANES) == 0 else 1
    tile = width // steps

    def copies(i):
        k, colour = units[i]
        if not adds:
            todo = [(o_buf.at[k, colour], outs[0].at[k, colour])]
        else:
            each, length = n_out // len(units), outs[0].shape[0]
            todo = [
                (o_buf.at[k, colour, length * j : length * (j + 1)], outs[i * each + j])
                for j in range(each)
            ]
        return [pltpu.make_async_copy(a, b, o_sem.at[i, j]) for j, (a, b) in enumerate(todo)]

    def unit(i, _):
        k, colour = i // 2, i % 2
        offset = k + k // 2 if count > 1 else offsets[0]

        @pl.when(k == 0)
        def _():
            pltpu.make_async_copy(w_buf.at[colour], w_buf.at[colour], w_sem.at[colour]).wait()

        if adds:
            there = r_buf[0].at[k, colour]
            pltpu.make_async_copy(there, there, r_sem.at[k, colour]).wait()
        h = h_ref[colour, offset].reshape(-1, ff)

        def column(t, _):
            at = pl.ds(pl.multiple_of(t * tile, LANES), tile)
            part = jnp.dot(h, w_buf[colour, :, at], preferred_element_type=jnp.float32)
            part = part.reshape(4, -1, tile)
            if adds:
                part = part + r_buf[0][k, colour, :, :, at].astype(jnp.float32)
            o_buf[k, colour, :, :, at] = part.astype(jnp.bfloat16)
            return 0

        lax.fori_loop(0, steps, column, 0)
        for u in range(2 * count):

            @pl.when(i == u)
            def _(u=u):
                for copy in copies(u):
                    copy.start()

        return 0

    lax.fori_loop(0, 2 * count, unit, 0)
    for u in range(2 * count):
        for copy in copies(u):
            copy.wait()


def down_call(place, hidden, down_mat, offsets, received):
    adds = received is not None
    rows, ff = hidden.shape[3:]
    width = down_mat.shape[1] // 4
    count = len(offsets)
    any_spec = pl.BlockSpec(memory_space=pl.ANY)
    whole = (count, 2, 4, rows, width)
    parts = 2 if offsets == (2,) else 1
    piece = jax.ShapeDtypeStruct((4 // parts, rows, width), jnp.bfloat16)
    moved = 2 * 2 * count * 4 * rows * width
    return pl.pallas_call(
        functools.partial(down_kernel, offsets, adds),
        out_shape=[piece] * (2 * count * parts) if adds else [jax.ShapeDtypeStruct(whole, jnp.bfloat16)],
        in_specs=[
            pl.BlockSpec(memory_space=pltpu.SMEM),
            pl.BlockSpec(memory_space=pltpu.VMEM),
            any_spec,
        ]
        + [any_spec] * adds,
        out_specs=[any_spec] * (2 * count * parts if adds else 1),
        scratch_shapes=[pltpu.VMEM((2, ff, width), jnp.bfloat16)]
        + [pltpu.VMEM(whole, jnp.bfloat16)] * (1 + adds)
        + [
            pltpu.SemaphoreType.DMA((2,)),
            pltpu.SemaphoreType.DMA((2 * count, 2)),
            pltpu.SemaphoreType.DMA((count, 2)),
        ],
        compiler_params=pltpu.CompilerParams(vmem_limit_bytes=20 * 2**20),
        cost_estimate=pl.CostEstimate(
            flops=2 * count * 8 * rows * ff * width,
            bytes_accessed=moved * (2 if adds else 1),
            transcendentals=0,
        ),
        name="down_add" if adds else "down_send",
    )(place, hidden, down_mat, *([received] if adds else []))


def step(tokens, routes, gate_scores, w_gate, w_up, w_down):
    tok_rows, model_width = tokens.shape
    half = model_width // 2
    core = lax.axis_index("c")
    expert = lax.axis_index(("y", "x", "c")).astype(jnp.int32)
    place = jnp.stack([core.astype(jnp.int32), expert])

    experts = lax.axis_size(("y", "x", "c"))
    named = routes[:, :, None] == jnp.arange(experts, dtype=jnp.int32)
    weights = jnp.sum(jnp.where(named, gate_scores[:, :, None], 0.0), axis=1)
    top = lax.reduce_precision(weights, 8, 7)
    pad = jnp.zeros((tok_rows, LANES // 2 - experts), jnp.float32)
    tile = jnp.concatenate([top, pad, weights - top, pad], axis=1).astype(jnp.bfloat16)

    first, second = tokens[:, :half], tokens[:, half:]
    mine = jnp.concatenate([tile, by_core(core, first, second)], axis=1)
    theirs = jnp.concatenate([tile, by_core(core, second, first)], axis=1)
    other = shift(theirs, "c", 1)
    block = by_core(
        core, jnp.concatenate([mine, other], axis=0), jnp.concatenate([other, mine], axis=0)
    )

    n_z = lax.axis_size("z")
    cut = LANES + half // 2
    column = jnp.broadcast_to(block, (n_z, *block.shape))
    column = lax.all_to_all(column, "z", split_axis=0, concat_axis=0, tiled=True)
    column = column.reshape(-1, block.shape[1])
    first = far_gather(near_gather(column[:, :cut], "x"), "y")
    second = far_gather(near_gather(column[:, cut:], "y"), "x")
    spots, sources = [], []
    for side in range(2):
        for colour, found in enumerate((first, second)):
            for offset, row, piece in found:
                at = offset * found[0][2].shape[0] + row
                spots.append((side, colour, at, len(sources), 0, piece.shape[0]))
                sources.append(shift(piece, "c", 1) if side else piece)
    down_mat = w_down[0]
    hidden, far_sent = hidden_call(place, tuple(spots), sources, w_gate[0], w_up[0], down_mat)

    groups = ((2,), (0, 1, 3))
    far_got = shift(far_sent, "c", 1)
    sent = down_call(place, hidden, down_mat, groups[1], None)[0]
    across = down_call(place, hidden, down_mat, groups[0], far_got)
    got = shift(sent, "c", 1)
    others = down_call(place, hidden, down_mat, groups[1], got)
    sums = []
    for colour, (near, far) in enumerate((("x", "y"), ("y", "x"))):
        own, succ, prev = others[colour::2]
        low, high = across[2 * colour : 2 * colour + 2]
        line = far_reduce(own, succ, low, high, prev, far)
        sums.append(near_reduce(line[0], line[1], line[2], line[3], near))
    column = jnp.concatenate(sums, axis=1).reshape(n_z, -1, half)
    column = lax.all_to_all(column, "z", split_axis=0, concat_axis=0, tiled=True)
    total = added(*[column[k] for k in range(n_z)])

    mine = by_core(core, total[:tok_rows], total[tok_rows:])
    theirs = by_core(core, total[tok_rows:], total[:tok_rows])
    other = shift(theirs, "c", 1)
    return by_core(
        core, jnp.concatenate([mine, other], axis=1), jnp.concatenate([other, mine], axis=1)
    )


def solution(mesh):
    grid = Mesh(mesh.devices.reshape(8, 4, 4, 2), ("z", "y", "x", "c"))
    every = ("z", "y", "x", "c")
    plane = ("y", "x", "c")
    return jax.shard_map(
        step,
        mesh=grid,
        in_specs=(
            P(every, None),
            P(every, None),
            P(every, None),
            P(plane, None, "z"),
            P(plane, None, "z"),
            P(plane, "z", None),
        ),
        out_specs=P(every, None),
        check_vma=False,
    )
```

```python
import functools

import jax
import jax.numpy as jnp
from jax import lax
from jax.experimental import pallas as pl
from jax.experimental.pallas import tpu as pltpu
from jax.sharding import Mesh, PartitionSpec as P


LANES = 128


def shift(value, axis, step):
    n = lax.axis_size(axis)
    return lax.ppermute(value, axis, [(i, (i + step) % n) for i in range(n)])


def near_gather(own, axis):
    return jnp.concatenate([own, shift(own, axis, -1), shift(own, axis, 2), shift(own, axis, 1)])


def near_reduce(own, succ, across, prev, axis):
    return added(own, shift(succ, axis, 1), shift(across, axis, 2), shift(prev, axis, -1))


def far_gather(own, axis):
    n = lax.axis_size(axis)
    half = own.shape[0] // 2
    pieces = [(0, 0, own)]
    prev = succ = own
    for k in range(1, n // 2):
        prev, succ = shift(prev, axis, 1), shift(succ, axis, -1)
        pieces += [(k, 0, succ), (n - k, 0, prev)]
    low, high = shift(prev[:half], axis, 1), shift(succ[half:], axis, -1)
    return pieces + [(n // 2, 0, low), (n // 2, half, high)]


def far_reduce(own, succ, low, high, prev, axis):
    half = low.shape[0]
    got_low = shift(low, axis, 1)
    got_high = shift(high, axis, -1)
    to_succ = jnp.concatenate([added(succ[:half], got_low), succ[half:]], axis=0)
    to_prev = jnp.concatenate([prev[:half], added(prev[half:], got_high)], axis=0)
    return added(own, shift(to_succ, axis, 1), shift(to_prev, axis, -1))


def added(*terms):
    total = terms[0].astype(jnp.float32)
    for term in terms[1:]:
        total = total + term.astype(jnp.float32)
    return total.astype(jnp.bfloat16)


def by_core(core, if_zero, if_one):
    return jnp.where(core == 0, if_zero, if_one)


def early_kernel(count, spots, place_ref, *refs):
    sources, (gate_ref, up_ref, acc, x_buf, w_buf, x_sem, w_sem) = refs[:count], refs[count:]
    lines, width = x_buf.shape[2:]
    ff = gate_ref.shape[1]
    core = place_ref[0]
    for colour in range(2):
        part = pl.ds(pl.multiple_of((2 * core + colour) * width, LANES), width)
        for k, ref in enumerate((gate_ref, up_ref)):
            pltpu.make_async_copy(
                ref.at[part, :], w_buf.at[colour, :, k * ff : (k + 1) * ff], w_sem.at[colour]
            ).start()
        for i, (which, slot) in enumerate(spots):
            if which == colour:
                skip = sources[i].shape[1] - width
                pltpu.make_async_copy(
                    sources[i].at[:, skip : skip + width], x_buf.at[colour, slot], x_sem.at[colour, slot]
                ).start()

    def step(i, _):
        colour, slot = i // 3, i % 3

        @pl.when(slot == 0)
        def _():
            pltpu.make_async_copy(w_buf.at[colour], w_buf.at[colour], w_sem.at[colour]).wait()

        there = x_buf.at[colour, slot]
        pltpu.make_async_copy(there, there, x_sem.at[colour, slot]).wait()
        at = pl.ds(pl.multiple_of((slot + slot // 2) * lines, 8), lines)
        acc[colour, at, :] = jnp.dot(
            x_buf[colour, slot], w_buf[colour], preferred_element_type=jnp.float32
        )
        return 0

    lax.fori_loop(0, 6, step, 0)


def early_call(place, spots, sources, gate_mat, up_mat):
    lines = sources[0].shape[0]
    ff = gate_mat.shape[1]
    width = gate_mat.shape[0] // 4
    any_spec = pl.BlockSpec(memory_space=pl.ANY)
    return pl.pallas_call(
        functools.partial(early_kernel, len(sources), spots),
        out_shape=jax.ShapeDtypeStruct((2, 4 * lines, 2 * ff), jnp.float32),
        in_specs=[pl.BlockSpec(memory_space=pltpu.SMEM)] + [any_spec] * (len(sources) + 2),
        out_specs=pl.BlockSpec(memory_space=pltpu.VMEM),
        scratch_shapes=[
            pltpu.VMEM((2, 3, lines, width), jnp.bfloat16),
            pltpu.VMEM((2, width, 2 * ff), jnp.bfloat16),
            pltpu.SemaphoreType.DMA((2, 3)),
            pltpu.SemaphoreType.DMA((2,)),
        ],
        compiler_params=pltpu.CompilerParams(vmem_limit_bytes=52 * 2**20),
        cost_estimate=pl.CostEstimate(
            flops=12 * lines * width * 2 * ff, bytes_accessed=9 * 2**20, transcendentals=0
        ),
        name="early",
    )(place, *sources, gate_mat, up_mat)


def hidden_kernel(count, spots, place_ref, *refs):
    sources, refs = refs[:count], refs[count:]
    gate_ref, up_ref, down_ref, early_ref, out_ref, sent_ref, x_buf, w_buf, acc, named = refs[:10]
    d_buf, o_buf, x_sem, w_sem, named_sem, d_sem, o_sem, acc_sem = refs[10:]
    lines, width = x_buf.shape[2:]
    rows = lines // 4
    ff = gate_ref.shape[1]
    core, expert = place_ref[0], place_ref[1]
    for side in range(2):
        half = core if side == 0 else 1 - core
        for colour in range(2):
            part = pl.ds(pl.multiple_of((2 * half + colour) * width, LANES), width)
            for k, ref in enumerate((gate_ref, up_ref)):
                pltpu.make_async_copy(
                    ref.at[part, :],
                    w_buf.at[2 * side + colour, :, k * ff : (k + 1) * ff],
                    w_sem.at[2 * side + colour],
                ).start()
        for which, colour, first, source, begin, length in spots:
            if which == side and (side == 1 or first // sources[0].shape[0] == 2):
                skip = sources[source].shape[1] - width
                block, row = first // lines, first % lines
                pltpu.make_async_copy(
                    sources[source].at[begin : begin + length, skip : skip + width],
                    x_buf.at[2 * side + colour, block, row : row + length],
                    x_sem.at[2 * side + colour, block],
                ).start()
    for side, colour, first, source, begin, length in spots:
        if side == 0 and colour == 0:
            pltpu.make_async_copy(
                sources[source].at[begin : begin + length, :LANES],
                named.at[first // lines, first % lines : first % lines + length],
                named_sem,
            ).start()

    for colour in range(2):
        part = pl.ds(pl.multiple_of((2 * (1 - core) + colour) * width, LANES), width)
        pltpu.make_async_copy(down_ref.at[:, part], d_buf.at[colour], d_sem.at[colour]).start()

    kept = ((0, 2), (3, 1))
    for begin, size in kept:
        at = slice(begin * lines, (begin + size) * lines)
        pltpu.make_async_copy(early_ref.at[:, at], acc.at[:, at], acc_sem.at[size - 1]).start()

    def step(i, _):
        early = i < 2
        group = jnp.where(early, i, 2 + (i - 2) // 4)
        block = jnp.where(early, 2, (i - 2) % 4)
        colour = group % 2

        @pl.when(early | (i == 2) | (i == 6))
        def _():
            pltpu.make_async_copy(w_buf.at[group], w_buf.at[group], w_sem.at[group]).wait()

        @pl.when(i == 2)
        def _():
            for begin, size in kept:
                there = acc.at[:, begin * lines : (begin + size) * lines]
                pltpu.make_async_copy(there, there, acc_sem.at[size - 1]).wait()

        there = x_buf.at[group, block]
        pltpu.make_async_copy(there, there, x_sem.at[group, block]).wait()
        part = jnp.dot(x_buf[group, block], w_buf[group], preferred_element_type=jnp.float32)
        at = pl.ds(pl.multiple_of(block * lines, 8), lines)
        acc[colour, at, :] = jnp.where(early, part, part + acc[colour, at, :])
        return 0

    lax.fori_loop(0, 10, step, 0)
    pltpu.make_async_copy(named, named, named_sem).wait()
    lane = lax.broadcasted_iota(jnp.int32, (LANES, ff), 0)
    chosen = ((lane == expert) | (lane == expert + LANES // 2)).astype(jnp.bfloat16)

    def finish(offset, _):
        weight = jnp.dot(named[offset], chosen, preferred_element_type=jnp.float32)
        for j in range(4):
            theirs = pl.ds(pl.multiple_of(j * lines + offset * rows, 8), rows)
            mine = pl.ds(pl.multiple_of(offset * lines + j * rows, 8), rows)
            total = acc[0, mine, :] + acc[1, theirs, :]
            gate, up = total[:, :ff], total[:, ff:]
            act = gate / (1.0 + jnp.exp(-gate)) * up * weight[j * rows : (j + 1) * rows]
            act = act.astype(jnp.bfloat16)
            out_ref[0, offset, j] = act
            out_ref[1, j, offset] = act
        return 0

    lax.fori_loop(0, 4, finish, 0)

    steps = 2 if width % (4 * LANES) == 0 else 1
    tile = width // steps
    for colour in range(2):
        pltpu.make_async_copy(d_buf.at[colour], d_buf.at[colour], d_sem.at[colour]).wait()

    def column(i, _):
        colour = i // steps
        at = pl.ds(pl.multiple_of(i % steps * tile, LANES), tile)
        h = out_ref[colour, 2].reshape(lines, ff)
        part = jnp.dot(h, d_buf[colour, :, at], preferred_element_type=jnp.float32)
        o_buf[0, colour, :, :, at] = part.reshape(4, rows, tile).astype(jnp.bfloat16)
        return 0

    lax.fori_loop(0, 2 * steps, column, 0)
    copy = pltpu.make_async_copy(o_buf, sent_ref, o_sem)
    copy.start()
    copy.wait()


def hidden_call(place, spots, sources, gate_mat, up_mat, down_mat, early):
    lines = sources[0].shape[0]
    rows = lines // 4
    ff = gate_mat.shape[1]
    width = gate_mat.shape[0] // 4
    any_spec = pl.BlockSpec(memory_space=pl.ANY)
    return pl.pallas_call(
        functools.partial(hidden_kernel, len(sources), spots),
        out_shape=[
            jax.ShapeDtypeStruct((2, 4, 4, rows, ff), jnp.bfloat16),
            jax.ShapeDtypeStruct((1, 2, 4, rows, width), jnp.bfloat16),
        ],
        in_specs=[pl.BlockSpec(memory_space=pltpu.SMEM)] + [any_spec] * (len(sources) + 4),
        out_specs=[pl.BlockSpec(memory_space=pltpu.VMEM), any_spec],
        scratch_shapes=[
            pltpu.VMEM((4, 4, lines, width), jnp.bfloat16),
            pltpu.VMEM((4, width, 2 * ff), jnp.bfloat16),
            pltpu.VMEM((2, 4 * lines, 2 * ff), jnp.float32),
            pltpu.VMEM((4, lines, LANES), jnp.bfloat16),
            pltpu.VMEM((2, ff, width), jnp.bfloat16),
            pltpu.VMEM((1, 2, 4, rows, width), jnp.bfloat16),
            pltpu.SemaphoreType.DMA((4, 4)),
            pltpu.SemaphoreType.DMA((4,)),
            pltpu.SemaphoreType.DMA,
            pltpu.SemaphoreType.DMA((2,)),
            pltpu.SemaphoreType.DMA,
            pltpu.SemaphoreType.DMA((2,)),
        ],
        compiler_params=pltpu.CompilerParams(vmem_limit_bytes=36 * 2**20),
        cost_estimate=pl.CostEstimate(
            flops=2 * 16 * rows * gate_mat.shape[0] * 2 * ff,
            bytes_accessed=24 * 2**20,
            transcendentals=0,
        ),
        name="hidden",
    )(place, *sources, gate_mat, up_mat, down_mat, early)


def down_kernel(offsets, adds, place_ref, h_ref, w_ref, *refs):
    recv_ref = refs[0] if adds else None
    refs = refs[1:] if adds else refs
    count = len(offsets)
    n_out = len(refs) - 6 if adds else 1
    outs = refs[:n_out]
    w_buf, o_buf, *r_buf, w_sem, o_sem, r_sem = refs[n_out:]
    ff, width = w_buf.shape[1:]
    half = place_ref[0] if adds else 1 - place_ref[0]
    for colour in range(2):
        columns = pl.ds(pl.multiple_of((half * 2 + colour) * width, LANES), width)
        pltpu.make_async_copy(w_ref.at[:, columns], w_buf.at[colour], w_sem.at[colour]).start()
    units = [(k, colour) for k in range(count) for colour in range(2)]
    for k, colour in units if adds else ():
        pltpu.make_async_copy(recv_ref.at[k, colour], r_buf[0].at[k, colour], r_sem.at[k, colour]).start()
    steps = 2 if width % (4 * LANES) == 0 else 1
    tile = width // steps

    def copies(i):
        k, colour = units[i]
        if not adds:
            todo = [(o_buf.at[k, colour], outs[0].at[k, colour])]
        else:
            each, length = n_out // len(units), outs[0].shape[0]
            todo = [
                (o_buf.at[k, colour, length * j : length * (j + 1)], outs[i * each + j])
                for j in range(each)
            ]
        return [pltpu.make_async_copy(a, b, o_sem.at[i, j]) for j, (a, b) in enumerate(todo)]

    def unit(i, _):
        k, colour = i // 2, i % 2
        offset = k + k // 2 if count > 1 else offsets[0]

        @pl.when(k == 0)
        def _():
            pltpu.make_async_copy(w_buf.at[colour], w_buf.at[colour], w_sem.at[colour]).wait()

        if adds:
            there = r_buf[0].at[k, colour]
            pltpu.make_async_copy(there, there, r_sem.at[k, colour]).wait()
        h = h_ref[colour, offset].reshape(-1, ff)

        def column(t, _):
            at = pl.ds(pl.multiple_of(t * tile, LANES), tile)
            part = jnp.dot(h, w_buf[colour, :, at], preferred_element_type=jnp.float32)
            part = part.reshape(4, -1, tile)
            if adds:
                part = part + r_buf[0][k, colour, :, :, at].astype(jnp.float32)
            o_buf[k, colour, :, :, at] = part.astype(jnp.bfloat16)
            return 0

        lax.fori_loop(0, steps, column, 0)
        for u in range(2 * count):

            @pl.when(i == u)
            def _(u=u):
                for copy in copies(u):
                    copy.start()

        return 0

    lax.fori_loop(0, 2 * count, unit, 0)
    for u in range(2 * count):
        for copy in copies(u):
            copy.wait()


def down_call(place, hidden, down_mat, offsets, received):
    adds = received is not None
    rows, ff = hidden.shape[3:]
    width = down_mat.shape[1] // 4
    count = len(offsets)
    any_spec = pl.BlockSpec(memory_space=pl.ANY)
    whole = (count, 2, 4, rows, width)
    parts = 2 if offsets == (2,) else 1
    piece = jax.ShapeDtypeStruct((4 // parts, rows, width), jnp.bfloat16)
    moved = 2 * 2 * count * 4 * rows * width
    return pl.pallas_call(
        functools.partial(down_kernel, offsets, adds),
        out_shape=[piece] * (2 * count * parts) if adds else [jax.ShapeDtypeStruct(whole, jnp.bfloat16)],
        in_specs=[
            pl.BlockSpec(memory_space=pltpu.SMEM),
            pl.BlockSpec(memory_space=pltpu.VMEM),
            any_spec,
        ]
        + [any_spec] * adds,
        out_specs=[any_spec] * (2 * count * parts if adds else 1),
        scratch_shapes=[pltpu.VMEM((2, ff, width), jnp.bfloat16)]
        + [pltpu.VMEM(whole, jnp.bfloat16)] * (1 + adds)
        + [
            pltpu.SemaphoreType.DMA((2,)),
            pltpu.SemaphoreType.DMA((2 * count, 2)),
            pltpu.SemaphoreType.DMA((count, 2)),
        ],
        compiler_params=pltpu.CompilerParams(vmem_limit_bytes=20 * 2**20),
        cost_estimate=pl.CostEstimate(
            flops=2 * count * 8 * rows * ff * width,
            bytes_accessed=moved * (2 if adds else 1),
            transcendentals=0,
        ),
        name="down_add" if adds else "down_send",
    )(place, hidden, down_mat, *([received] if adds else []))


def step(tokens, routes, gate_scores, w_gate, w_up, w_down):
    tok_rows, model_width = tokens.shape
    half = model_width // 2
    core = lax.axis_index("c")
    expert = lax.axis_index(("y", "x", "c")).astype(jnp.int32)
    place = jnp.stack([core.astype(jnp.int32), expert])

    experts = lax.axis_size(("y", "x", "c"))
    named = routes[:, :, None] == jnp.arange(experts, dtype=jnp.int32)
    weights = jnp.sum(jnp.where(named, gate_scores[:, :, None], 0.0), axis=1)
    top = lax.reduce_precision(weights, 8, 7)
    pad = jnp.zeros((tok_rows, LANES // 2 - experts), jnp.float32)
    tile = jnp.concatenate([top, pad, weights - top, pad], axis=1).astype(jnp.bfloat16)

    first, second = tokens[:, :half], tokens[:, half:]
    mine = jnp.concatenate([tile, by_core(core, first, second)], axis=1)
    theirs = jnp.concatenate([tile, by_core(core, second, first)], axis=1)
    other = shift(theirs, "c", 1)
    block = by_core(
        core, jnp.concatenate([mine, other], axis=0), jnp.concatenate([other, mine], axis=0)
    )

    n_z = lax.axis_size("z")
    cut = LANES + half // 2
    column = jnp.broadcast_to(block, (n_z, *block.shape))
    column = lax.all_to_all(column, "z", split_axis=0, concat_axis=0, tiled=True)
    column = column.reshape(-1, block.shape[1])
    first = far_gather(near_gather(column[:, :cut], "x"), "y")
    second = far_gather(near_gather(column[:, cut:], "y"), "x")
    spots, sources = [], []
    for side in range(2):
        for colour, found in enumerate((first, second)):
            for offset, row, piece in found:
                at = offset * found[0][2].shape[0] + row
                spots.append((side, colour, at, len(sources), 0, piece.shape[0]))
                sources.append(shift(piece, "c", 1) if side else piece)
    down_mat = w_down[0]
    parts = [(c, (0, 1, 3).index(k), p) for c, f in enumerate((first, second)) for k, _, p in f if k != 2]
    early = early_call(
        place, tuple(p[:2] for p in parts), [p[2] for p in parts], w_gate[0], w_up[0]
    )
    hidden, far_sent = hidden_call(
        place, tuple(spots), sources, w_gate[0], w_up[0], down_mat, early
    )

    groups = ((2,), (0, 1, 3))
    far_got = shift(far_sent, "c", 1)
    sent = down_call(place, hidden, down_mat, groups[1], None)[0]
    across = down_call(place, hidden, down_mat, groups[0], far_got)
    got = shift(sent, "c", 1)
    others = down_call(place, hidden, down_mat, groups[1], got)
    sums = []
    for colour, (near, far) in enumerate((("x", "y"), ("y", "x"))):
        own, succ, prev = others[colour::2]
        low, high = across[2 * colour : 2 * colour + 2]
        line = far_reduce(own, succ, low, high, prev, far)
        sums.append(near_reduce(line[0], line[1], line[2], line[3], near))
    column = jnp.concatenate(sums, axis=1).reshape(n_z, -1, half)
    column = lax.all_to_all(column, "z", split_axis=0, concat_axis=0, tiled=True)
    total = added(*[column[k] for k in range(n_z)])

    mine = by_core(core, total[:tok_rows], total[tok_rows:])
    theirs = by_core(core, total[tok_rows:], total[:tok_rows])
    other = shift(theirs, "c", 1)
    return by_core(
        core, jnp.concatenate([mine, other], axis=1), jnp.concatenate([other, mine], axis=1)
    )


def solution(mesh):
    grid = Mesh(mesh.devices.reshape(8, 4, 4, 2), ("z", "y", "x", "c"))
    every = ("z", "y", "x", "c")
    plane = ("y", "x", "c")
    return jax.shard_map(
        step,
        mesh=grid,
        in_specs=(
            P(every, None),
            P(every, None),
            P(every, None),
            P(plane, None, "z"),
            P(plane, None, "z"),
            P(plane, "z", None),
        ),
        out_specs=P(every, None),
        check_vma=False,
    )
```
